32 devices in a mesh: wide: 8 (over y, x, core), narrow: 4 (over z).
Axes of the slice: x: 2, y: 2, z: 4, core: 2. Of those that a mesh axis runs over, the one named last changes fastest.
Arguments:
- first_state: float32 [2, 32768, 1024], P(None, ('wide', 'narrow')), may hold values from -100 to 100
- second_state: float32 [2, 32768, 1024], P(None, ('wide', 'narrow')), may hold values from -200 to 200
- place_first: int32 [32768], replicated, may hold values from 0 to 32767, as said below
- place_second: int32 [32768], replicated, may hold values from 0 to 32767, as said below
Outputs:
- aligned: float32 [2, 32768, 1024], P(None, ('wide', 'narrow'))
- intersection: float32 [2], replicated
- norms: float32 [2], replicated
The draws below stay inside these ranges and needn't reach their ends.
Inputs may be any that keep to these rules, and one draw needn't show every extreme that they name: Each of place_first and place_second maps a logical block index to a storage block index by a permutation of the index's bits. Every logical bit that selects a device (the high bits of a storage index above its position within a device) in one state's order selects a block within a device in the other's, so each device holds exactly 32 blocks of the second state that the first state's order places on any given device. `place_second`: drawn together with place_first under the rule stated there.
All inputs are finite; a program needn't handle non-finite values.
Results may differ from the reference program's by a relative error of at most 0.00002.
Values sent between devices are 32-bit elements; how exact they have to be, the bound alone decides.
A program may use at most 128 MiB of HBM per device.

```python
import math
import jax
import jax.numpy as jnp
from jax import lax

BLOCK = 1024
BLOCKS_DEV = 1024
BLOCKS = 32768
AMPS = 33554432


def block_maps(key):
    block_bits = int(BLOCKS).bit_length() - 1
    global_bits = int(BLOCKS // BLOCKS_DEV).bit_length() - 1
    local_bits = block_bits - global_bits
    sigma = jax.random.permutation(jax.random.fold_in(key, 11), block_bits).astype(jnp.int32)
    device_first = sigma[:global_bits]
    device_second = sigma[global_bits:2 * global_bits]
    others = sigma[2 * global_bits:]
    order_first = jax.random.permutation(jax.random.fold_in(key, 12), local_bits).astype(jnp.int32)
    order_second = jax.random.permutation(jax.random.fold_in(key, 13), local_bits).astype(jnp.int32)
    local_first = jnp.concatenate([device_second, others])[order_first]
    local_second = jnp.concatenate([device_first, others])[order_second]
    map_first = jnp.concatenate([local_first, device_first]).astype(jnp.int32)
    map_second = jnp.concatenate([local_second, device_second]).astype(jnp.int32)
    return (map_first, map_second)


def storage_of(logical, bit_map):
    block_bits = int(BLOCKS).bit_length() - 1
    store = jnp.zeros_like(logical)
    for level in range(block_bits):
        store = store + jnp.left_shift(jnp.right_shift(logical, bit_map[level]) & 1, level)
    return store.astype(jnp.int32)


def logical_of(store, bit_map):
    block_bits = int(BLOCKS).bit_length() - 1
    logical = jnp.zeros_like(store)
    for level in range(block_bits):
        logical = logical + jnp.left_shift(jnp.right_shift(store, level) & 1, bit_map[level])
    return logical.astype(jnp.int32)


def block_scale(key, expo):
    steps = jnp.arange(BLOCKS, dtype=jnp.float32) / float(max(BLOCKS - 1, 1))
    rising = jnp.exp(expo * math.log(3.0) * steps)
    spread = jnp.exp(jax.random.uniform(key, (BLOCKS,), jnp.float32, 0.0, 0.5 * math.log(10.0)))
    return rising * spread


def base_normals(key):
    return jnp.clip(jax.random.normal(jax.random.fold_in(key, 31), (2, BLOCKS, BLOCK), jnp.float32), -6.0, 6.0)


def draw_place_first(key, part):
    map_first, map_second = block_maps(key)
    return storage_of(jnp.arange(BLOCKS, dtype=jnp.int32), map_first)


def draw_place_second(key, part):
    map_first, map_second = block_maps(key)
    return storage_of(jnp.arange(BLOCKS, dtype=jnp.int32), map_second)


def draw_first_state(key, part):
    expo = 0.5
    scale_first = block_scale(jax.random.fold_in(key, 21), expo)
    return base_normals(key) * scale_first[None, :, None]


def draw_second_state(key, part):
    expo = 0.5
    map_first, map_second = block_maps(key)
    logical = logical_of(jnp.arange(BLOCKS, dtype=jnp.int32), map_second)
    rows_first = storage_of(logical, map_first)
    shared = jnp.take(base_normals(key), rows_first, axis=1)
    angles = jax.random.uniform(jax.random.fold_in(key, 41), (BLOCKS,), jnp.float32, 0.3, 1.2)
    cosine = jnp.cos(angles)[:, None]
    sine = jnp.sin(angles)[:, None]
    turned = jnp.stack([cosine * shared[0] - sine * shared[1], sine * shared[0] + cosine * shared[1]])
    noise = jnp.clip(jax.random.normal(jax.random.fold_in(key, 32), (2, BLOCKS, BLOCK), jnp.float32), -6.0, 6.0)
    scale_second = block_scale(jax.random.fold_in(key, 22), expo)
    return (0.6 * turned + 0.8 * noise) * scale_second[None, :, None]


def setup_inputs(seed: int = 0) -> dict:
    key_of = jax.random.split(jax.random.key(seed), 5)
    first_state = draw_first_state(jax.random.fold_in(key_of[4], 71), 0)
    second_state = draw_second_state(jax.random.fold_in(key_of[4], 71), 0)
    place_first = draw_place_first(jax.random.fold_in(key_of[4], 71), 0)
    place_second = draw_place_second(jax.random.fold_in(key_of[4], 71), 0)
    return dict(first_state=first_state, second_state=second_state, place_first=place_first, place_second=place_second)


def reference(first_state, second_state, place_first, place_second):
    index_list = jnp.arange(BLOCKS, dtype=jnp.int32)
    logical_first = jnp.zeros((BLOCKS,), jnp.int32).at[place_first].set(index_list)
    source_blocks = place_second[logical_first].astype(jnp.int32)
    gathered = jnp.take(second_state, source_blocks, axis=1)
    amp_total = float(AMPS)
    first_sq = jnp.sum(lax.optimization_barrier(jnp.sum(first_state * first_state, axis=2)))
    second_sq = jnp.sum(lax.optimization_barrier(jnp.sum(second_state * second_state, axis=2)))
    real_sum = jnp.sum(lax.optimization_barrier(jnp.sum(first_state[0] * gathered[0] + first_state[1] * gathered[1], axis=1)))
    imag_sum = jnp.sum(lax.optimization_barrier(jnp.sum(first_state[0] * gathered[1] - first_state[1] * gathered[0], axis=1)))
    mean_first = first_sq / amp_total
    mean_second = second_sq / amp_total
    aligned = gathered / jnp.sqrt(mean_second + 1e-06)
    intersection = jnp.stack([real_sum, imag_sum]) / amp_total / jnp.sqrt((mean_first + 1e-06) * (mean_second + 1e-06))
    norms = jnp.stack([mean_first, mean_second])
    return (aligned, intersection, norms)
```

```python
import functools

import jax
import jax.numpy as jnp
from jax import lax
from jax.experimental import pallas as pl
from jax.experimental.pallas import tpu as pltpu
from jax.sharding import PartitionSpec as P

MESH = pl.DeviceIdType.MESH
SUB = 8
LANE = 128


def bit_places(place, levels):
    powers = jnp.stack([place[1 << level] for level in range(levels)])
    found = jnp.zeros_like(powers)
    for spot in range(levels):
        found = found + (jnp.right_shift(powers, spot) & 1) * spot
    return found


def maps(place_first, place_second, blocks_dev, devices):
    levels = (blocks_dev * devices).bit_length() - 1
    local_bits = blocks_dev.bit_length() - 1
    share_bits = (blocks_dev // devices).bit_length() - 1
    pf = bit_places(place_first, levels)
    ps = bit_places(place_second, levels)
    f_local = pf < local_bits
    s_local = ps < local_bits
    both = (f_local & s_local).astype(jnp.int32)
    rank = jnp.cumsum(both) - both
    out_pos = jnp.where(f_local, rank, pf - local_bits + share_bits)
    in_pos = jnp.where(s_local, rank, ps - local_bits + share_bits)
    t = jnp.arange(blocks_dev, dtype=jnp.int32)
    send = jnp.zeros_like(t)
    land = jnp.zeros_like(t)
    back = jnp.zeros_like(t)
    for level in range(levels):
        send += jnp.where(s_local[level], ((t >> out_pos[level]) & 1) << jnp.where(s_local[level], ps[level], 0), 0)
        land += jnp.where(f_local[level], ((t >> in_pos[level]) & 1) << jnp.where(f_local[level], pf[level], 0), 0)
        back += jnp.where(f_local[level], ((t >> jnp.where(f_local[level], pf[level], 0)) & 1) << in_pos[level], 0)
    return send, land, back


def row_of(part, slot, blocks_dev):
    return part * (blocks_dev * SUB) + (slot // SUB) * (SUB * SUB) + lax.rem(slot, SUB)


def exchange(sizes, blocks_dev, share, send_map, land_map, first_hbm, second_hbm, recv_hbm, stats_out,
             first, second, outgoing, arrived, stats, totals,
             load_sem, send_sem, recv_sem, keep_sem, sq_send, sq_recv, dot_send, dot_recv):
    wide_count, narrow_count = sizes
    devices = wide_count * narrow_count
    me_w = lax.axis_index("wide")
    me_n = lax.axis_index("narrow")
    me = me_w * narrow_count + me_n

    load_second = pltpu.make_async_copy(second_hbm, second, load_sem.at[0])
    load_first = pltpu.make_async_copy(first_hbm, first, load_sem.at[1])
    load_second.start()
    load_first.start()

    def partner(step):
        other_w = lax.rem(me_w + step // narrow_count, wide_count)
        other_n = lax.rem(me_n + lax.rem(step, narrow_count), narrow_count)
        return other_w, other_n

    def giver(step):
        other_w = lax.rem(me_w + wide_count - step // narrow_count, wide_count)
        other_n = lax.rem(me_n + narrow_count - lax.rem(step, narrow_count), narrow_count)
        return other_w * narrow_count + other_n

    barrier = pltpu.get_barrier_semaphore()

    @pl.loop(1, devices)
    def _(step):
        pl.semaphore_signal(barrier, inc=1, device_id=partner(step), device_id_type=MESH)

    load_second.wait()
    pl.semaphore_wait(barrier, devices - 1)

    def block_copy(step):
        return pltpu.make_async_remote_copy(
            src_ref=outgoing.at[step], dst_ref=arrived.at[step],
            send_sem=send_sem.at[step], recv_sem=recv_sem.at[step],
            device_id=partner(step), device_id_type=MESH)

    def pack(step):
        other_w, other_n = partner(step)
        base = (other_w * narrow_count + other_n) * share

        def row(k, carry):
            slot = send_map[base + k]
            for part in range(2):
                start = row_of(part, slot, blocks_dev)
                outgoing[step, part, k] = second[pl.ds(start, SUB, stride=SUB), :]
            return carry

        lax.fori_loop(0, share, row, 0, unroll=min(8, share))

    pack(1)

    @pl.loop(2, devices)
    def _(step):
        pack(step)
        block_copy(step - 1).start()

    own_base = me * share

    def own_row(k, carry):
        slot = send_map[own_base + k]
        for part in range(2):
            start = row_of(part, slot, blocks_dev)
            arrived[0, part, k] = second[pl.ds(start, SUB, stride=SUB), :]
        return carry

    lax.fori_loop(0, share, own_row, 0, unroll=min(8, share))
    block_copy(devices - 1).start()

    load_first.wait()
    rows = 2 * blocks_dev * SUB
    chunk = 16 * SUB

    def squares(i, carry):
        at = pl.multiple_of(i * chunk, chunk)
        a = first[pl.ds(at, chunk), :].reshape(chunk // SUB, SUB, LANE)
        b = second[pl.ds(at, chunk), :].reshape(chunk // SUB, SUB, LANE)
        return carry[0] + jnp.sum(a * a, axis=0), carry[1] + jnp.sum(b * b, axis=0)

    zero = jnp.zeros((SUB, LANE), jnp.float32)
    sq_first, sq_second = lax.fori_loop(0, rows // chunk, squares, (zero, zero))
    stats[0, 0] = jnp.broadcast_to(jnp.sum(sq_first, axis=0, keepdims=True), (SUB, LANE))
    stats[0, 1] = jnp.broadcast_to(jnp.sum(sq_second, axis=0, keepdims=True), (SUB, LANE))

    def keep(step):
        return pltpu.make_async_copy(arrived.at[step], recv_hbm.at[giver(step)], keep_sem.at[step])

    def dots(step, carry):
        base = giver(step) * share

        def row(k, carry):
            real, imag = carry
            slot = land_map[base + k]
            f_re = first[pl.ds(row_of(0, slot, blocks_dev), SUB, stride=SUB), :]
            f_im = first[pl.ds(row_of(1, slot, blocks_dev), SUB, stride=SUB), :]
            g_re = arrived[step, 0, k]
            g_im = arrived[step, 1, k]
            return real + (f_re * g_re + f_im * g_im), imag + (f_re * g_im - f_im * g_re)

        return lax.fori_loop(0, share, row, carry, unroll=min(8, share))

    keep(0).start()
    carry = dots(0, (zero, zero))

    def sq_copy(step):
        return pltpu.make_async_remote_copy(
            src_ref=stats.at[0], dst_ref=totals.at[0, step],
            send_sem=sq_send.at[step], recv_sem=sq_recv.at[step],
            device_id=partner(step), device_id_type=MESH)

    def dot_copy(step):
        return pltpu.make_async_remote_copy(
            src_ref=stats.at[1], dst_ref=totals.at[1, step],
            send_sem=dot_send.at[step], recv_sem=dot_recv.at[step],
            device_id=partner(step), device_id_type=MESH)

    @pl.loop(1, devices)
    def _(step):
        sq_copy(step).start()

    def take(step, carry):
        block_copy(step).wait_recv()
        keep(step).start()
        return dots(step, carry)

    real, imag = lax.fori_loop(1, devices, take, carry)
    stats[1, 0] = jnp.broadcast_to(jnp.sum(real, axis=0, keepdims=True), (SUB, LANE))
    stats[1, 1] = jnp.broadcast_to(jnp.sum(imag, axis=0, keepdims=True), (SUB, LANE))

    @pl.loop(1, devices)
    def _(step):
        block_copy(step).wait_send()
        sq_copy(step).wait()
        keep(step).wait()

    @pl.loop(1, devices)
    def _(step):
        dot_copy(step).start()

    keep(0).wait()
    totals[0, 0] = stats[0]
    totals[1, 0] = stats[1]

    @pl.loop(1, devices)
    def _(step):
        dot_copy(step).wait()

    def add(device, carry):
        gone_w = lax.rem(me_w + wide_count - device // narrow_count, wide_count)
        gone_n = lax.rem(me_n + narrow_count - lax.rem(device, narrow_count), narrow_count)
        step = gone_w * narrow_count + gone_n
        return carry + totals[:, step]

    stats_out[...] = lax.fori_loop(0, devices, add, jnp.zeros((2, 2, SUB, LANE), jnp.float32))


def unpack(blocks_dev, groups, back_map, scale, recv_hbm, out, arrived, sem):
    at = pl.program_id(0)

    @pl.when(at == 0)
    def _():
        copy = pltpu.make_async_copy(recv_hbm, arrived, sem)
        copy.start()
        copy.wait()

    share = arrived.shape[2]
    factor = scale[0]

    def group(i, carry):
        base = pl.multiple_of(i * (SUB * SUB), SUB * SUB)
        for r in range(SUB):
            index = back_map[(at * groups + i) * SUB + r]
            device = index // share
            k = lax.rem(index, share)
            for part in range(2):
                out[part, pl.ds(base + r, SUB, stride=SUB), :] = arrived[device, part, k] * factor
        return carry

    lax.fori_loop(0, groups, group, 0)


def local(first_state, second_state, place_first, place_second):
    blocks_dev = first_state.shape[1]
    block = first_state.shape[2]
    wide_count = lax.axis_size("wide")
    narrow_count = lax.axis_size("narrow")
    devices = wide_count * narrow_count
    share = blocks_dev // devices
    send_map, land_map, back_map = maps(place_first, place_second, blocks_dev, devices)

    def tiles(state):
        split = state.reshape(2, blocks_dev // SUB, SUB, block // LANE, LANE)
        return split.transpose(0, 1, 3, 2, 4).reshape(2 * blocks_dev * SUB, LANE)

    packed = (devices, 2, share, SUB, LANE)
    recv, totals = pl.pallas_call(
        functools.partial(exchange, (wide_count, narrow_count), blocks_dev, share),
        out_shape=(jax.ShapeDtypeStruct(packed, jnp.float32),
                   jax.ShapeDtypeStruct((2, 2, SUB, LANE), jnp.float32)),
        in_specs=[pl.BlockSpec(memory_space=pltpu.SMEM)] * 2 + [pl.BlockSpec(memory_space=pl.ANY)] * 2,
        out_specs=(pl.BlockSpec(memory_space=pl.ANY), pl.BlockSpec(memory_space=pltpu.VMEM)),
        scratch_shapes=[
            pltpu.VMEM((2 * blocks_dev * SUB, LANE), jnp.float32),
            pltpu.VMEM((2 * blocks_dev * SUB, LANE), jnp.float32),
            pltpu.VMEM(packed, jnp.float32),
            pltpu.VMEM(packed, jnp.float32),
            pltpu.VMEM((2, 2, SUB, LANE), jnp.float32),
            pltpu.VMEM((2, devices, 2, SUB, LANE), jnp.float32),
            pltpu.SemaphoreType.DMA((2,)),
        ] + [pltpu.SemaphoreType.DMA((devices,))] * 7,
        compiler_params=pltpu.CompilerParams(
            collective_id=0, has_side_effects=True, vmem_limit_bytes=48 * 1024 * 1024),
        name="exchange",
    )(send_map, land_map, tiles(first_state), tiles(second_state))

    amp_total = float(blocks_dev * devices * block)
    sums = jnp.sum(totals[:, :, 0, :], axis=-1) / amp_total
    mean_first = sums[0, 0]
    mean_second = sums[0, 1]
    scale = 1.0 / jnp.sqrt(mean_second + 1e-06)
    steps = 8
    groups = blocks_dev // SUB // steps
    aligned = pl.pallas_call(
        functools.partial(unpack, blocks_dev, groups),
        out_shape=jax.ShapeDtypeStruct((2, blocks_dev * SUB, LANE), jnp.float32),
        grid=(steps,),
        in_specs=[pl.BlockSpec(memory_space=pltpu.SMEM)] * 2 + [pl.BlockSpec(memory_space=pl.ANY)],
        out_specs=pl.BlockSpec((2, groups * SUB * SUB, LANE), lambda i: (0, i, 0)),
        scratch_shapes=[pltpu.VMEM(packed, jnp.float32), pltpu.SemaphoreType.DMA],
        name="unpack",
    )(back_map, scale.reshape(1), recv)
    aligned = aligned.reshape(2, blocks_dev // SUB, block // LANE, SUB, LANE)
    aligned = aligned.transpose(0, 1, 3, 2, 4).reshape(2, blocks_dev, block)
    intersection = sums[1] / jnp.sqrt((mean_first + 1e-06) * (mean_second + 1e-06))
    norms = jnp.stack([mean_first, mean_second])
    return (aligned, intersection, norms)


def solution(mesh):
    return jax.shard_map(
        local,
        mesh=mesh,
        in_specs=(P(None, ("wide", "narrow"), None), P(None, ("wide", "narrow"), None), P(), P()),
        out_specs=(P(None, ("wide", "narrow"), None), P(), P()),
        check_vma=False,
    )
```

```python
import functools

import jax
import jax.numpy as jnp
from jax import lax
from jax.experimental import pallas as pl
from jax.experimental.pallas import tpu as pltpu
from jax.sharding import PartitionSpec as P

MESH = pl.DeviceIdType.MESH
SUB = 8
LANE = 128


def row_weight(one_hot):
    return jnp.where(one_hot < SUB, one_hot, one_hot * SUB)


def bits(count):
    return count.bit_length() - 1


def table(ref, base, weights):
    ref[base] = jnp.int32(0)
    for level, weight in enumerate(weights):
        for low in range(1 << level):
            ref[base + (1 << level) + low] = ref[base + low] + weight


def build_tables(place_f, place_s, blocks_dev, devices, share, rows_out, rows_in, back):
    levels = bits(blocks_dev * devices)
    zero = jnp.int32(0)
    dev_out = [zero] * bits(devices)
    dev_in = [zero] * bits(devices)
    k_out = [zero] * bits(share)
    k_in = [zero] * bits(share)
    slot_back = [zero] * bits(blocks_dev)
    unit = jnp.int32(1)
    for level in range(levels):
        f = place_f(level)
        s = place_s(level)
        f_dev = f >> bits(blocks_dev)
        s_dev = s >> bits(blocks_dev)
        both = (f_dev == 0) & (s_dev == 0)
        for j in range(bits(devices)):
            dev_out[j] = dev_out[j] + jnp.where(f_dev == (1 << j), row_weight(s), 0)
            dev_in[j] = dev_in[j] + jnp.where(s_dev == (1 << j), row_weight(f), 0)
        for i in range(bits(share)):
            here = both & (unit == (1 << i))
            k_out[i] = k_out[i] + jnp.where(here, row_weight(s), 0)
            k_in[i] = k_in[i] + jnp.where(here, row_weight(f), 0)
        packed = jnp.where(both, unit * SUB, s_dev * (2 * share * SUB))
        for p in range(bits(blocks_dev)):
            slot_back[p] = slot_back[p] + jnp.where(f == (1 << p), packed, 0)
        unit = jnp.where(both, unit * 2, unit)
    table(rows_out, 0, dev_out)
    table(rows_out, devices, k_out)
    table(rows_in, 0, dev_in)
    table(rows_in, devices, k_in)
    table(back, 0, slot_back[:bits(SUB)])
    table(back, SUB, slot_back[bits(SUB):])


def exchange(sizes, blocks_dev, share, place_first, place_second, first_hbm, second_hbm,
             recv_hbm, stats_out, back,
             first, second, outgoing, arrived, stats, totals, powers, rows_out, rows_in,
             load_sem, place_sem, send_sem, recv_sem, keep_sem, sq_send, sq_recv, dot_send, dot_recv):
    wide_count, narrow_count = sizes
    devices = wide_count * narrow_count
    levels = bits(blocks_dev * devices)
    me_w = lax.axis_index("wide")
    me_n = lax.axis_index("narrow")
    me = me_w * narrow_count + me_n
    part_rows = blocks_dev * SUB

    lines = [0] + [1 << line for line in range(levels - bits(LANE))]
    fetches = []
    for which, place in enumerate((place_first, place_second)):
        for at, line in enumerate(lines):
            fetches.append(pltpu.make_async_copy(
                place.at[pl.ds(line, 1), :], powers.at[which, pl.ds(at, 1), :],
                place_sem.at[which * len(lines) + at]))
    load_second = pltpu.make_async_copy(second_hbm, second, load_sem.at[0])
    load_first = pltpu.make_async_copy(first_hbm, first, load_sem.at[1])
    for fetch in fetches:
        fetch.start()
    load_second.start()

    def partner(offset):
        return (jnp.bitwise_xor(me_w, offset // narrow_count),
                jnp.bitwise_xor(me_n, lax.rem(offset, narrow_count)))

    def other(offset):
        other_w, other_n = partner(offset)
        return other_w * narrow_count + other_n

    barrier = pltpu.get_barrier_semaphore()

    @pl.loop(1, devices)
    def _(offset):
        pl.semaphore_signal(barrier, inc=1, device_id=partner(offset), device_id_type=MESH)

    for fetch in fetches:
        fetch.wait()

    def place_of(which):
        def entry(level):
            if (1 << level) < LANE:
                return powers[which, 0, 1 << level]
            return powers[which, 1 + level - bits(LANE), 0]
        return entry

    build_tables(place_of(0), place_of(1), blocks_dev, devices, share, rows_out, rows_in, back)
    load_second.wait()
    load_first.start()
    pl.semaphore_wait(barrier, devices - 1)

    last = narrow_count - 1
    inner = (me_n != 0) & (me_n != last)
    flip = jnp.where(lax.rem(me_w, 2) == 1, wide_count - 2, 0)

    def offset_of(seq):
        turn = seq // wide_count
        far = jnp.where(inner, jnp.where(turn == 0, last, turn), turn + 1)
        away = jnp.bitwise_xor(lax.rem(seq, wide_count), flip) * narrow_count + far
        near = (seq - wide_count * last + 1) * narrow_count
        return jnp.where(turn < last, away, near)

    outside = wide_count * last

    def block_copy(offset):
        return pltpu.make_async_remote_copy(
            src_ref=outgoing.at[offset], dst_ref=arrived.at[offset],
            send_sem=send_sem.at[offset], recv_sem=recv_sem.at[offset],
            device_id=partner(offset), device_id_type=MESH)

    def pack(offset, out):
        base = rows_out[other(offset)]

        def row(k, carry):
            start = base + rows_out[devices + k]
            for part in range(2):
                out[offset, part, k] = second[pl.ds(start + part * part_rows, SUB, stride=SUB), :]
            return carry

        lax.fori_loop(0, share, row, 0, unroll=min(8, share))

    pack(offset_of(0), outgoing)

    @pl.loop(1, devices - 1)
    def _(seq):
        pack(offset_of(seq), outgoing)

        @pl.when(seq <= outside)
        def _():
            block_copy(offset_of(seq - 1)).start()

    pack(0, arrived)

    load_first.wait()
    chunk = 16 * SUB

    def squares(i, carry):
        at = pl.multiple_of(i * chunk, chunk)
        a = first[pl.ds(at, chunk), :].reshape(chunk // SUB, SUB, LANE)
        b = second[pl.ds(at, chunk), :].reshape(chunk // SUB, SUB, LANE)
        return carry[0] + jnp.sum(a * a, axis=0), carry[1] + jnp.sum(b * b, axis=0)

    zero = jnp.zeros((SUB, LANE), jnp.float32)
    sq_first, sq_second = lax.fori_loop(0, 2 * part_rows // chunk, squares, (zero, zero))
    stats[0, 0] = sq_first
    stats[0, 1] = sq_second

    def keep(offset):
        return pltpu.make_async_copy(arrived.at[offset], recv_hbm.at[other(offset)], keep_sem.at[offset])

    def dots(offset, carry):
        base = rows_in[other(offset)]

        def row(k, carry):
            real, imag = carry
            start = base + rows_in[devices + k]
            f_re = first[pl.ds(start, SUB, stride=SUB), :]
            f_im = first[pl.ds(start + part_rows, SUB, stride=SUB), :]
            g_re = arrived[offset, 0, k]
            g_im = arrived[offset, 1, k]
            return real + (f_re * g_re + f_im * g_im), imag + (f_re * g_im - f_im * g_re)

        return lax.fori_loop(0, share, row, carry, unroll=min(8, share))

    keep(0).start()
    carry = dots(0, (zero, zero))

    def sum_copy(kind, sems, offset):
        return pltpu.make_async_remote_copy(
            src_ref=stats.at[kind], dst_ref=totals.at[kind, offset],
            send_sem=sems[0].at[offset], recv_sem=sems[1].at[offset],
            device_id=partner(offset), device_id_type=MESH)

    sq_copy = functools.partial(sum_copy, 0, (sq_send, sq_recv))
    dot_copy = functools.partial(sum_copy, 1, (dot_send, dot_recv))

    @pl.loop(1, devices)
    def _(offset):
        sq_copy(offset).start()

    def take(offset, carry):
        block_copy(offset).wait_recv()
        keep(offset).start()
        return dots(offset, carry)

    def take_and_send(seq, carry):
        block_copy(offset_of(outside + seq)).start()
        return take(offset_of_arrival(seq), carry)

    def offset_of_arrival(seq):
        turn = seq // wide_count
        far = jnp.where(inner, jnp.where(turn == 0, last, turn), turn + 1)
        return jnp.bitwise_xor(lax.rem(seq, wide_count), flip) * narrow_count + far

    carry = lax.fori_loop(0, wide_count - 1, take_and_send, carry)
    carry = take(offset_of_arrival(wide_count - 1), carry)
    carry = lax.fori_loop(outside, devices - 1, lambda seq, c: take(offset_of(seq), c), carry)
    real, imag = lax.fori_loop(
        wide_count, outside, lambda seq, c: take(offset_of_arrival(seq), c), carry)
    stats[1, 0] = real
    stats[1, 1] = imag

    @pl.loop(1, devices)
    def _(offset):
        block_copy(offset).wait_send()
        sq_copy(offset).wait()
        keep(offset).wait()

    @pl.loop(1, devices)
    def _(offset):
        dot_copy(offset).start()

    keep(0).wait()
    totals[0, 0] = stats[0]
    totals[1, 0] = stats[1]

    @pl.loop(1, devices)
    def _(offset):
        dot_copy(offset).wait()

    def add(device, carry):
        return carry + totals[:, jnp.bitwise_xor(me, device)]

    stats_out[...] = lax.fori_loop(0, devices, add, jnp.zeros((2, 2, SUB, LANE), jnp.float32))


def unpack(amp_total, groups, part_rows, back, stats, recv_hbm, out, intersection, norms, arrived, factor, sem):
    at = pl.program_id(0)

    @pl.when(at == 0)
    def _():
        copy = pltpu.make_async_copy(recv_hbm, arrived, sem)
        copy.start()

        def mean(kind, which):
            total = jnp.sum(stats[kind, which]) / amp_total
            return jnp.broadcast_to(total, (SUB, LANE))

        mean_first = mean(0, 0)
        mean_second = mean(0, 1)
        norms[0] = mean_first[0, 0]
        norms[1] = mean_second[0, 0]
        both = jnp.sqrt((mean_first + 1e-06) * (mean_second + 1e-06))
        for which in range(2):
            intersection[which] = (mean(1, which) / both)[0, 0]
        factor[...] = 1.0 / jnp.sqrt(mean_second + 1e-06)
        copy.wait()

    scale = factor[...]

    def group(i, carry):
        base = pl.multiple_of(i * (SUB * SUB), SUB * SUB)
        high = back[SUB + at * groups + i]
        for r in range(SUB):
            start = pl.multiple_of(high + back[r], SUB)
            for part in range(2):
                block = arrived[pl.ds(pl.multiple_of(start + part * part_rows, SUB), SUB), :]
                out[part, pl.ds(base + r, SUB, stride=SUB), :] = block * scale
        return carry

    lax.fori_loop(0, groups, group, 0, unroll=2)


def local(first_state, second_state, place_first, place_second):
    blocks_dev = first_state.shape[1]
    block = first_state.shape[2]
    wide_count = lax.axis_size("wide")
    narrow_count = lax.axis_size("narrow")
    devices = wide_count * narrow_count
    share = blocks_dev // devices
    lines = 1 + bits(blocks_dev * devices) - bits(LANE)

    def tiles(state):
        split = state.reshape(2, blocks_dev // SUB, SUB, block // LANE, LANE)
        return split.transpose(0, 1, 3, 2, 4).reshape(2 * blocks_dev * SUB, LANE)

    packed = (devices, 2, share, SUB, LANE)
    rows = (2 * blocks_dev * SUB, LANE)
    any_spec = pl.BlockSpec(memory_space=pl.ANY)
    smem_spec = pl.BlockSpec(memory_space=pltpu.SMEM)
    recv, stats, back = pl.pallas_call(
        functools.partial(exchange, (wide_count, narrow_count), blocks_dev, share),
        out_shape=(jax.ShapeDtypeStruct(packed, jnp.float32),
                   jax.ShapeDtypeStruct((2, 2, SUB, LANE), jnp.float32),
                   jax.ShapeDtypeStruct((SUB + blocks_dev // SUB,), jnp.int32)),
        in_specs=[any_spec] * 4,
        out_specs=(any_spec, pl.BlockSpec(memory_space=pltpu.VMEM), smem_spec),
        scratch_shapes=[
            pltpu.VMEM(rows, jnp.float32),
            pltpu.VMEM(rows, jnp.float32),
            pltpu.VMEM(packed, jnp.float32),
            pltpu.VMEM(packed, jnp.float32),
            pltpu.VMEM((2, 2, SUB, LANE), jnp.float32),
            pltpu.VMEM((2, devices, 2, SUB, LANE), jnp.float32),
            pltpu.SMEM((2, lines, LANE), jnp.int32),
            pltpu.SMEM((devices + share,), jnp.int32),
            pltpu.SMEM((devices + share,), jnp.int32),
            pltpu.SemaphoreType.DMA((2,)),
            pltpu.SemaphoreType.DMA((2 * lines,)),
        ] + [pltpu.SemaphoreType.DMA((devices,))] * 7,
        compiler_params=pltpu.CompilerParams(
            collective_id=0, has_side_effects=True, vmem_limit_bytes=48 * 1024 * 1024),
        name="exchange",
    )(place_first.reshape(-1, LANE), place_second.reshape(-1, LANE),
      tiles(first_state), tiles(second_state))

    steps = 8
    groups = blocks_dev // SUB // steps
    aligned, intersection, norms = pl.pallas_call(
        functools.partial(unpack, float(blocks_dev * devices * block), groups, share * SUB),
        out_shape=(jax.ShapeDtypeStruct((2, blocks_dev * SUB, LANE), jnp.float32),
                   jax.ShapeDtypeStruct((2,), jnp.float32),
                   jax.ShapeDtypeStruct((2,), jnp.float32)),
        grid=(steps,),
        in_specs=[smem_spec, pl.BlockSpec(memory_space=pltpu.VMEM), any_spec],
        out_specs=(pl.BlockSpec((2, groups * SUB * SUB, LANE), lambda i: (0, i, 0)), smem_spec, smem_spec),
        scratch_shapes=[pltpu.VMEM(rows, jnp.float32), pltpu.VMEM((SUB, LANE), jnp.float32),
                        pltpu.SemaphoreType.DMA],
        name="unpack",
    )(back, stats, recv.reshape(rows))
    aligned = aligned.reshape(2, blocks_dev // SUB, block // LANE, SUB, LANE)
    aligned = aligned.transpose(0, 1, 3, 2, 4).reshape(2, blocks_dev, block)
    return (aligned, intersection, norms)


def solution(mesh):
    return jax.shard_map(
        local,
        mesh=mesh,
        in_specs=(P(None, ("wide", "narrow"), None), P(None, ("wide", "narrow"), None), P(), P()),
        out_specs=(P(None, ("wide", "narrow"), None), P(), P()),
        check_vma=False,
    )
```
